32 devices in a mesh: seq: 8 (over z, x), head: 4 (over y, core).
Axes of the slice: x: 2, y: 2, z: 4, core: 2. Of those that a mesh axis runs over, the one named last changes fastest.
Arguments:
- queries: bfloat16 [8192, 4096], P('seq', 'head'), may hold values from -150 to 150
- keys: bfloat16 [8192, 4096], P('seq', 'head'), may hold values from -7 to 7
- values: bfloat16 [8192, 4096], P('seq', 'head'), may hold values from -6 to 6
- random_holder: int32 [32, 64, 3], P('head', 'seq'), may hold values from 0 to 7, all different within a row; in each aligned block of 8 rows (0 to 7, 8 to 15, ..., all dimensions but the last counted through in order) at most 3 rows name the same one
- random_offset: int32 [32, 64, 3], P('head', 'seq'), may hold values from 0 to 7
- keep: int32 [64], P('seq'), may hold values from 0 to 1, as said below
Outputs:
- packed: bfloat16 [8192, 4096], P('seq', 'head')
The draws below stay inside these ranges and needn't reach their ends.
Inputs may be any that keep to these rules, and one draw needn't show every extreme that they name: `random_holder`: for each head, the 8 query blocks of one index of seq name no index of seq more than 3 times over all their random entries; the 3 entries of one query block and head differ. `keep`: block j is kept where j % 8 == 0 or j % 8 == 7, and not kept where j % 8 == 1.
All inputs are finite; a program needn't handle non-finite values.
Results may differ from the reference program's by a relative error of at most 0.007.
Values may be sent and summed in bfloat16 or wider, within the bound.
A program may use at most 128 MiB of HBM per device.

```python
import math
import jax
import jax.numpy as jnp
import numpy as np
from jax import lax

H = 32
DH = 128
B = 128
G = 2
R = 3
BD = 8
NB = 64
L = 8192
MOST = 3
N_SEQ = 8


def paired_rows(key):
    base = jax.random.fold_in(key, 71)
    key_rows = jnp.clip(jax.random.normal(jax.random.fold_in(base, 1), (L, H * DH), jnp.float32), -6.0, 6.0)
    query_rows = jnp.clip(jax.random.normal(jax.random.fold_in(base, 2), (L, H * DH), jnp.float32), -6.0, 6.0)
    return (query_rows, key_rows)


def draw_queries(key, part):
    query_rows, key_rows = paired_rows(key)
    return query_rows.astype(jnp.bfloat16)


def draw_keys(key, part):
    query_rows, key_rows = paired_rows(key)
    return key_rows.astype(jnp.bfloat16)


def draw_keep(key, part):
    count = L // B
    rolled = jax.random.randint(jax.random.fold_in(key, 113), (count,), 0, 3)
    kept = (rolled == 0).astype(jnp.int32)
    position = jnp.arange(count, dtype=jnp.int32) % BD
    kept = jnp.where(position == 0, 1, kept)
    kept = jnp.where(position == BD - 1, 1, kept)
    kept = jnp.where(position == 1, 0, kept)
    return kept.astype(jnp.int32)


def plant(array, key, smallest, largest):
    extent = array.shape
    spot = [jax.random.randint(jax.random.fold_in(key, axis), (), 0, extent[axis]) for axis in range(len(extent))]
    array = array.at[tuple(spot)].set(smallest)
    longest = extent.index(max(extent))
    spot[longest] = (spot[longest] + 1) % extent[longest]
    return array.at[tuple(spot)].set(largest)


def levels(rng, shape, split, low, high):
    gain = 1.0
    for dim, shards_of in split:
        heights = jax.random.uniform(jax.random.fold_in(jax.random.fold_in(rng, 6), dim), (shards_of,), jnp.float32, low / len(split), high / len(split))
        gain = gain * jnp.repeat(jnp.exp(heights), shape[dim] // shards_of).reshape((-1,) + (1,) * (len(shape) - 1 - dim))
    return gain


def shared_out(rng, own, number, rows, number_of, top, limit, slope):
    sequence = jax.random.permutation(rng, number_of)
    heavy_load, usual = shares(number_of, rows * top, limit, slope, True), shares(number_of, rows * top, limit, slope, False)
    places = jnp.arange(number_of)

    def named(sizes, offset_by):
        used = int((sizes > 0).sum())
        fixed = max(1, used // 4)
        shifted = fixed + (places - fixed + offset_by * (used - fixed)) % max(1, number_of - fixed)
        return jnp.zeros((number_of,), jnp.int32).at[sequence[jnp.where(places < fixed, places, shifted)]].set(jnp.asarray(sizes, jnp.int32))

    sizes = jnp.where(number % 4 == 0, named(heavy_load, number // 4), named(usual, number - number // 4 - 1))
    mixed = jax.random.permutation(jax.random.fold_in(own, 3), number_of)
    source_of, sink = mixed[0:number_of // 2 * 2:2], mixed[1:number_of // 2 * 2:2]
    slack = jnp.minimum(sizes[source_of] - 1, limit - sizes[sink]) // 2
    slack = jnp.where((source_of == sequence[0]) | (sink == sequence[0]) | (sizes[sink] == 0), 0, jnp.maximum(slack, 0))
    shifted = jax.random.randint(jax.random.fold_in(own, 4), (number_of // 2,), 0, 1 << 20) % (slack + 1)
    sizes = sizes.at[source_of].add(-shifted).at[sink].add(shifted)
    labels = jnp.searchsorted(jnp.cumsum(sizes), jnp.arange(rows * top), side="right").astype(jnp.int32)
    table = labels.reshape(top, rows).T
    table = table[jax.random.permutation(jax.random.fold_in(own, 1), rows)]
    offset_by = jax.random.randint(jax.random.fold_in(own, 2), (rows, 1), 0, top)
    return jnp.take_along_axis(table, (jnp.arange(top)[None, :] + offset_by) % top, axis=1)


def shares(amount, total, limit, skew, full):
    weights = [(1 << 20) // math.isqrt(standing ** skew) + 1 for standing in range(1, amount + 1)]
    largest = limit if full else min(limit, max(-(-total // amount), total * weights[0] // sum(weights)))
    least = 1 if total - largest >= amount - 1 else 0
    counts, spare = [largest] + [least] * (amount - 1), total - largest - least * (amount - 1)
    while spare > 0:
        movable = [i for i in range(1, amount) if counts[i] < largest] or [i for i in range(1, amount) if counts[i] < limit]
        whole, left = sum([weights[i] for i in movable]), spare
        for i in movable:
            more = min(limit - counts[i], max(1, left * weights[i] // whole), spare)
            counts[i] = counts[i] + more
            spare = spare - more
    return np.array(counts)


def bell_draw(rng, dims, deviation, bound, split=(), kind=jnp.bfloat16):
    drawn = jax.random.normal(rng, dims, jnp.float32) * deviation
    if len(split) > 0:
        drawn = levels(rng, dims, split, -0.22, 0.18) * drawn
    return jnp.clip(drawn, min=-bound, max=bound).astype(kind)


def setup_inputs(seed: int = 0) -> dict:
    key_of = jax.random.split(jax.random.key(seed), 7)
    queries = draw_queries(jax.random.fold_in(key_of[6], 71), 0)
    keys = draw_keys(jax.random.fold_in(key_of[6], 71), 0)
    values = bell_draw(key_of[2], (L, H * DH), 1.0, 6.0, ((0, 8), (1, 4)))
    random_holder_keys = jax.random.split(jax.random.fold_in(key_of[3], 1), H * NB // BD)
    random_holder_turns = jax.random.permutation(jax.random.fold_in(key_of[3], 3), H * NB // BD)
    random_holder = jax.vmap(lambda own, number: shared_out(jax.random.fold_in(key_of[3], 2), own, number, BD, N_SEQ, R, MOST, 2))(random_holder_keys, random_holder_turns).reshape((H, NB, R))
    random_offset = plant(jax.random.randint(key_of[4], (H, NB, R), 0, BD), jax.random.fold_in(key_of[4], 1), 0, BD - 1).astype(jnp.int32)
    keep = draw_keep(jax.random.fold_in(key_of[6], 71), 0)
    return {"queries": queries, "keys": keys, "values": values, "random_holder": random_holder, "random_offset": random_offset, "keep": keep}


neg_big = -1.0e30


def reference(queries, keys, values, random_holder, random_offset, keep):
    score_scale = 1.0 / (DH ** 0.5)
    query_blocks = queries.reshape(NB, B, H, DH)
    key_blocks = keys.reshape(NB, B, H, DH)
    value_blocks = values.reshape(NB, B, H, DH)
    head_idx = jnp.arange(H, dtype=jnp.int32)[:, None]

    def one_block(block_idx):
        left = jnp.maximum(block_idx - 1, 0)
        right = jnp.minimum(block_idx + 1, NB - 1)
        common = jnp.concatenate((jnp.stack((left, block_idx, right)).astype(jnp.int32), jnp.arange(G, dtype=jnp.int32)))
        common_keys = jnp.transpose(key_blocks[common], (0, 2, 1, 3))
        common_values = jnp.transpose(value_blocks[common], (0, 2, 1, 3))
        chosen = (random_holder[:, block_idx] * BD + random_offset[:, block_idx]).astype(jnp.int32)
        rand_keys = jnp.transpose(key_blocks[chosen, :, head_idx, :], (1, 0, 2, 3))
        rand_values = jnp.transpose(value_blocks[chosen, :, head_idx, :], (1, 0, 2, 3))
        tile_keys = jnp.concatenate((common_keys, rand_keys), axis=0).astype(jnp.float32)
        tile_values = jnp.concatenate((common_values, rand_values), axis=0).astype(jnp.float32)
        live = jnp.concatenate((jnp.stack((block_idx > 0, block_idx >= 0, block_idx < NB - 1)), jnp.ones((G + R,), dtype=bool)))
        query_tile = jnp.transpose(query_blocks[block_idx], (1, 0, 2)).astype(jnp.float32)
        scores = jnp.einsum('hqd,thkd->thqk', query_tile, tile_keys) * score_scale
        row_max = jnp.max(scores, axis=-1)
        weights = jnp.exp(scores - row_max[..., None]).astype(jnp.bfloat16).astype(jnp.float32)
        row_sum = jnp.sum(weights, axis=-1)
        summed = jnp.einsum('thqk,thkd->thqd', weights, tile_values)
        live_b = live[:, None, None]
        overall = jnp.max(jnp.where(live_b, row_max, neg_big), axis=0)
        factor = jnp.where(live_b, jnp.exp(row_max - overall[None]), 0.0)
        numer = jnp.sum(factor[..., None] * summed, axis=0)
        denom = jnp.sum(factor * row_sum, axis=0)
        result = numer / denom[..., None]
        return jnp.transpose(result, (1, 0, 2)).reshape(B, H * DH).astype(jnp.bfloat16)

    attended = lax.map(one_block, jnp.arange(NB, dtype=jnp.int32))
    keep_i = keep.astype(jnp.int32)
    local_rank = (jnp.cumsum(keep_i) - keep_i).astype(jnp.int32)
    place = jnp.where(keep_i > 0, local_rank, NB).astype(jnp.int32)
    packed = jnp.zeros((NB + 1, B, H * DH), jnp.bfloat16).at[place].set(attended)
    return packed[:NB].reshape(L, H * DH)
```

```python
import functools
import math

import jax
import jax.numpy as jnp
from jax import lax
from jax.experimental import pallas as pl
from jax.experimental.pallas import tpu as pltpu
from jax.sharding import PartitionSpec as P

DH = 128
B = 128
G = 2
R = 3

neg_big = -1e30
ANYWHERE = pltpu.CompilerParams(
    dimension_semantics=("arbitrary",), vmem_limit_bytes=60 * 1024 * 1024
)


def halo(block, axis, width):
    count = lax.axis_size(axis)
    forward = [(i, i + 1) for i in range(count - 1)]
    backward = [(target, source) for source, target in forward]
    low = lax.ppermute(block[-width:], axis, forward)
    high = lax.ppermute(block[:width], axis, backward)
    return jnp.concatenate([low, high], axis=0)


def broadcast(block, axis, source):
    block = jnp.where(lax.axis_index(axis) == source, block, jnp.zeros_like(block))
    return lax.psum(block, axis)


def pick_kernel(cap, head_ref, block_ref, k_ref, v_ref, out_ref):
    dest = pl.program_id(0)

    @pl.loop(0, cap)
    def _(j):
        rows = pl.ds(pl.multiple_of(block_ref[dest, j] * B, B), B)
        cols = pl.ds(pl.multiple_of(head_ref[dest, j] * DH, DH), DH)
        out_ref[j, 0] = k_ref[rows, cols]
        out_ref[j, 1] = v_ref[rows, cols]


def pick(keys, values, heads, blocks, seq_count, cap):
    whole = pl.BlockSpec(keys.shape, lambda d, *_: (0, 0))
    return pl.pallas_call(
        functools.partial(pick_kernel, cap),
        out_shape=jax.ShapeDtypeStruct((seq_count * cap, 2, B, DH), keys.dtype),
        grid_spec=pltpu.PrefetchScalarGridSpec(
            num_scalar_prefetch=2,
            grid=(seq_count,),
            in_specs=[whole, whole],
            out_specs=pl.BlockSpec((cap, 2, B, DH), lambda d, *_: (d, 0, 0, 0)),
        ),
        compiler_params=ANYWHERE,
    )(heads, blocks, keys, values)


def attend_kernel(
    blk_dev,
    keep_ref,
    slot_ref,
    live_ref,
    where_ref,
    q_ref,
    k_ref,
    v_ref,
    hk_ref,
    hv_ref,
    gk_ref,
    gv_ref,
    rand_ref,
    out_ref,
):
    scale = 1.0 / math.sqrt(DH)
    head = pl.program_id(0)
    out_ref[...] = jnp.zeros_like(out_ref)

    def tile(ref, halo_ref, i):
        if i < 0:
            return halo_ref[:B]
        if i >= blk_dev:
            return halo_ref[B:]
        return ref[i * B : (i + 1) * B]

    def one(i):
        q = q_ref[i * B : (i + 1) * B]
        near = range(i - 1, i + 2)
        picks = [where_ref[(head * blk_dev + i) * R + r] for r in range(R)]
        k_parts = [
            jnp.concatenate([tile(k_ref, hk_ref, n) for n in near], axis=0),
            gk_ref[...],
            jnp.concatenate([rand_ref[p, 0] for p in picks], axis=0),
        ]
        v_parts = [
            jnp.concatenate([tile(v_ref, hv_ref, n) for n in near], axis=0),
            gv_ref[...],
            jnp.concatenate([rand_ref[p, 1] for p in picks], axis=0),
        ]
        scores = [
            lax.dot_general(
                q, k, (((1,), (1,)), ((), ())), preferred_element_type=jnp.float32
            )
            * scale
            for k in k_parts
        ]
        lanes = lax.broadcasted_iota(jnp.int32, scores[0].shape, 1)
        if i == 0:
            dead = jnp.logical_and(lanes < B, live_ref[0] == 0)
            scores[0] = jnp.where(dead, neg_big, scores[0])
        if i == blk_dev - 1:
            dead = jnp.logical_and(lanes >= 2 * B, live_ref[1] == 0)
            scores[0] = jnp.where(dead, neg_big, scores[0])
        peak = functools.reduce(
            jnp.maximum, [jnp.max(s, axis=-1, keepdims=True) for s in scores]
        )
        numer = jnp.zeros((B, DH), jnp.float32)
        denom = jnp.zeros((B, 1), jnp.float32)
        for s, v in zip(scores, v_parts):
            w = jnp.exp(s - peak).astype(jnp.bfloat16)
            denom = denom + jnp.sum(w.astype(jnp.float32), axis=-1, keepdims=True)
            numer = numer + jnp.dot(w, v, preferred_element_type=jnp.float32)
        rows = pl.ds(pl.multiple_of(slot_ref[i] * B, B), B)
        out_ref[rows, :] = (numer / denom).astype(out_ref.dtype)

    for i in range(blk_dev):
        pl.when(keep_ref[i] > 0)(functools.partial(one, i))


def attend(keep, slot, live, where, q, k, v, hk, hv, gk, gv, rand):
    tok_dev, width_dev = q.shape
    blk_dev, head_dev = tok_dev // B, width_dev // DH

    def column(rows):
        return pl.BlockSpec((rows, DH), lambda h, *_: (0, h))

    return pl.pallas_call(
        functools.partial(attend_kernel, blk_dev),
        out_shape=jax.ShapeDtypeStruct(q.shape, q.dtype),
        grid_spec=pltpu.PrefetchScalarGridSpec(
            num_scalar_prefetch=4,
            grid=(head_dev,),
            in_specs=[column(tok_dev)] * 3
            + [column(2 * B)] * 2
            + [column(G * B)] * 2
            + [pl.BlockSpec(rand.shape, lambda h, *_: (0, 0, 0, 0))],
            out_specs=column(tok_dev),
        ),
        compiler_params=ANYWHERE,
    )(keep, slot, live, where, q, k, v, hk, hv, gk, gv, rand)


def copy_kernel(order_ref, in_ref, out_ref):
    out_ref[...] = in_ref[...]


def take_blocks(blocks, order, cap):
    width = blocks.shape[1]
    return pl.pallas_call(
        copy_kernel,
        out_shape=jax.ShapeDtypeStruct((cap * B, width), blocks.dtype),
        grid_spec=pltpu.PrefetchScalarGridSpec(
            num_scalar_prefetch=1,
            grid=(cap,),
            in_specs=[pl.BlockSpec((B, width), lambda j, order: (order[j], 0))],
            out_specs=pl.BlockSpec((B, width), lambda j, order: (j, 0)),
        ),
        compiler_params=ANYWHERE,
    )(order, blocks)


def merge_kernel(kind_ref, from_ref, old_ref, new_ref, out_ref):
    kind = kind_ref[pl.program_id(0)]

    @pl.when(kind == 0)
    def _():
        out_ref[...] = old_ref[...]

    @pl.when(kind == 1)
    def _():
        out_ref[...] = jnp.zeros_like(out_ref)

    @pl.when(kind == 2)
    def _():
        out_ref[...] = new_ref[...]


def merge_blocks(old, new, kind, place):
    tok_dev, width = old.shape
    return pl.pallas_call(
        merge_kernel,
        out_shape=jax.ShapeDtypeStruct(old.shape, old.dtype),
        grid_spec=pltpu.PrefetchScalarGridSpec(
            num_scalar_prefetch=2,
            grid=(tok_dev // B,),
            in_specs=[
                pl.BlockSpec((B, width), lambda j, kind, place: (j, 0)),
                pl.BlockSpec((B, width), lambda j, kind, place: (place[j], 0)),
            ],
            out_specs=pl.BlockSpec((B, width), lambda j, kind, place: (j, 0)),
        ),
        compiler_params=ANYWHERE,
    )(kind, place, old, new)


def exclusive(flags, axis):
    return jnp.cumsum(flags, axis=axis) - flags


def first_at_least(caps, amount):
    return jnp.sum((amount > jnp.asarray(caps, jnp.int32)).astype(jnp.int32))


def body(queries, keys, values, random_holder, random_offset, keep):
    tok_dev, width_dev = queries.shape
    blk_dev = tok_dev // B
    head_dev = width_dev // DH
    seq_count = lax.axis_size("seq")
    head_count = lax.axis_size("head")
    me = lax.axis_index("seq")
    count_req = blk_dev * R
    total = head_dev * count_req
    i32 = jnp.int32

    code = random_holder * blk_dev + random_offset
    code = jnp.where((keep > 0)[None, :, None], code, -1).reshape(total)
    table = lax.all_gather(jnp.concatenate([code, keep]), ("seq", "head"))
    table = table.reshape(seq_count, head_count, total + blk_dev)
    keep_all = table[:, 0, total:].reshape(seq_count * blk_dev)
    codes = table[:, :, :total]
    devices = jnp.arange(seq_count, dtype=i32)

    halo_k, halo_v = halo(keys, "seq", B), halo(values, "seq", B)
    glob_k, glob_v = broadcast(jnp.stack((keys[: G * B], values[: G * B])), "seq", 0)

    named = jnp.where(codes >= 0, codes // blk_dev, -1)
    counts = jnp.sum((named[..., None] == devices).astype(i32), axis=2)
    most = jnp.max(counts)
    onehot = (named[me, lax.axis_index("head")][:, None] == devices).astype(i32)
    mine = exclusive(onehot, 0)
    my_slot = jnp.sum(mine * onehot, axis=1)
    my_holder = jnp.sum(onehot * devices, axis=1)

    group = codes[:, lax.axis_index("head")]
    asks = (named[:, lax.axis_index("head")] == me).astype(i32)
    order = exclusive(asks, 1)
    full = min(total, head_dev * max(2, (count_req + seq_count - 1) // seq_count))
    chosen = asks[..., None] * (order[..., None] == jnp.arange(full, dtype=i32)).astype(i32)
    ask_head = jnp.arange(total, dtype=i32) // count_req
    ask = jnp.where(group >= 0, group % blk_dev, 0) + ask_head[None] * blk_dev
    ask = jnp.sum(chosen * ask[..., None], axis=1)
    pick_head, pick_block = ask // blk_dev, ask % blk_dev

    rank = exclusive(keep_all, 0)
    slot = rank % blk_dev
    source = jnp.arange(seq_count * blk_dev, dtype=i32) // blk_dev
    distance = jnp.where(keep_all > 0, source - rank // blk_dev, 0)
    my_slots = lax.dynamic_slice_in_dim(slot, me * blk_dev, blk_dev)
    live = jnp.stack([me > 0, me < seq_count - 1]).astype(i32)

    caps = sorted({max(1, full * part // 12) for part in range(5, 13)})

    def gathered(cap):
        def run(q, k, v, hk, hv, gk, gv):
            picked = pick(k, v, pick_head, pick_block, seq_count, cap)
            replies = lax.all_to_all(picked, "seq", split_axis=0, concat_axis=0, tiled=True)
            where = jnp.minimum(my_holder * cap + my_slot, seq_count * cap - 1)
            return attend(keep, my_slots, live, where, q, k, v, hk, hv, gk, gv, replies)

        return run

    blocks = lax.switch(
        first_at_least(caps[:-1], most),
        [gathered(cap) for cap in caps],
        queries, keys, values, halo_k, halo_v, glob_k, glob_v,
    )

    slots = jnp.arange(blk_dev, dtype=i32)
    sizes = sorted({0, *range(blk_dev // 2 - 1, blk_dev + 1)})
    for bit_pos in range((seq_count - 1).bit_length()):
        stride = 2**bit_pos
        at = source - distance % stride
        moving = (keep_all > 0) & (distance // stride % 2 > 0)
        on_slot = ((slot[:, None] == slots) & moving[:, None]).astype(i32)
        on_device = (at[:, None] == devices).astype(i32)
        leaving = jnp.sum(on_device[:, :, None] * on_slot[:, None, :], axis=0)
        needed = jnp.max(jnp.sum(leaving, axis=1))
        nth = exclusive(leaving, 1)
        mine_out, mine_nth = leaving[me], nth[me]
        send = jnp.sum(
            mine_out[:, None] * (mine_nth[:, None] == slots).astype(i32) * slots[:, None], axis=0
        )
        far = jnp.minimum(me + stride, seq_count - 1)
        comes = jnp.where(me + stride < seq_count, leaving[far], 0)
        kind = jnp.where(comes > 0, 2, jnp.where(mine_out > 0, 1, 0)).astype(i32)
        place = jnp.where(comes > 0, nth[far], 0)
        all_pairs = [(i, i - stride) for i in range(stride, seq_count)]
        split = seq_count - stride // 2
        upper = [pair for pair in all_pairs if pair[0] >= split]
        halves = 2 * stride >= seq_count and 0 < len(upper) < len(all_pairs)

        def shifting(cap, pairs, send=send, kind=kind, place=place):
            def run(blocks):
                if cap == 0:
                    return blocks
                moved = lax.ppermute(take_blocks(blocks, send, cap), "seq", pairs)
                return merge_blocks(blocks, moved, kind, jnp.minimum(place, cap - 1))

            return run

        which = first_at_least(sizes[:-1], needed)
        runs = [shifting(cap, all_pairs) for cap in sizes]
        if halves:
            runs += [shifting(cap, upper) for cap in sizes]
            lower = jnp.sum(leaving * (devices < split)[:, None].astype(i32))
            which = which + jnp.where(lower > 0, 0, len(sizes))
        blocks = lax.switch(which, runs, blocks)
    return blocks


def solution(mesh):
    in_specs = (
        P("seq", "head"),
        P("seq", "head"),
        P("seq", "head"),
        P("head", "seq", None),
        P("head", "seq", None),
        P("seq"),
    )
    out_specs = P("seq", "head")
    return jax.shard_map(body, mesh=mesh, in_specs=in_specs, out_specs=out_specs, check_vma=False)
```

```python
import functools
import math

import jax
import jax.numpy as jnp
from jax import lax
from jax.experimental import pallas as pl
from jax.experimental.pallas import tpu as pltpu
from jax.sharding import PartitionSpec as P

DH = 128
B = 128
G = 2
R = 3

neg_big = -1e30
ANYWHERE = pltpu.CompilerParams(
    dimension_semantics=("arbitrary",), vmem_limit_bytes=60 * 1024 * 1024
)


def halo(block, axis, width):
    count = lax.axis_size(axis)
    forward = [(i, i + 1) for i in range(count - 1)]
    backward = [(target, source) for source, target in forward]
    low = lax.ppermute(block[-width:], axis, forward)
    high = lax.ppermute(block[:width], axis, backward)
    return jnp.concatenate([low, high], axis=0)


def broadcast(block, axis, source):
    block = jnp.where(lax.axis_index(axis) == source, block, jnp.zeros_like(block))
    return lax.psum(block, axis)


def pick_kernel(cap, head_ref, block_ref, k_ref, v_ref, out_ref):
    dest = pl.program_id(0)

    @pl.loop(0, cap)
    def _(j):
        rows = pl.ds(pl.multiple_of(block_ref[dest, j] * B, B), B)
        cols = pl.ds(pl.multiple_of(head_ref[dest, j] * DH, DH), DH)
        out_ref[j, 0] = k_ref[rows, cols]
        out_ref[j, 1] = v_ref[rows, cols]


def pick(keys, values, heads, blocks, seq_count, cap):
    whole = pl.BlockSpec(keys.shape, lambda d, *_: (0, 0))
    return pl.pallas_call(
        functools.partial(pick_kernel, cap),
        out_shape=jax.ShapeDtypeStruct((seq_count * cap, 2, B, DH), keys.dtype),
        grid_spec=pltpu.PrefetchScalarGridSpec(
            num_scalar_prefetch=2,
            grid=(seq_count,),
            in_specs=[whole, whole],
            out_specs=pl.BlockSpec((cap, 2, B, DH), lambda d, *_: (d, 0, 0, 0)),
        ),
        compiler_params=ANYWHERE,
    )(heads, blocks, keys, values)


def attend_kernel(
    blk_dev,
    keep_ref,
    slot_ref,
    live_ref,
    where_ref,
    q_ref,
    k_ref,
    v_ref,
    hk_ref,
    hv_ref,
    gk_ref,
    gv_ref,
    rand_ref,
    out_ref,
):
    scale = 1.0 / math.sqrt(DH)
    head = pl.program_id(0)
    out_ref[...] = jnp.zeros_like(out_ref)

    def tile(ref, halo_ref, i):
        if i < 0:
            return halo_ref[:B]
        if i >= blk_dev:
            return halo_ref[B:]
        return ref[i * B : (i + 1) * B]

    def one(i):
        q = q_ref[i * B : (i + 1) * B]
        near = range(i - 1, i + 2)
        picks = [where_ref[(head * blk_dev + i) * R + r] for r in range(R)]
        k_parts = [
            jnp.concatenate([tile(k_ref, hk_ref, n) for n in near], axis=0),
            gk_ref[...],
            jnp.concatenate([rand_ref[p, 0] for p in picks], axis=0),
        ]
        v_parts = [
            jnp.concatenate([tile(v_ref, hv_ref, n) for n in near], axis=0),
            gv_ref[...],
            jnp.concatenate([rand_ref[p, 1] for p in picks], axis=0),
        ]
        scores = [
            lax.dot_general(
                q, k, (((1,), (1,)), ((), ())), preferred_element_type=jnp.float32
            )
            * scale
            for k in k_parts
        ]
        lanes = lax.broadcasted_iota(jnp.int32, scores[0].shape, 1)
        if i == 0:
            dead = jnp.logical_and(lanes < B, live_ref[0] == 0)
            scores[0] = jnp.where(dead, neg_big, scores[0])
        if i == blk_dev - 1:
            dead = jnp.logical_and(lanes >= 2 * B, live_ref[1] == 0)
            scores[0] = jnp.where(dead, neg_big, scores[0])
        peak = functools.reduce(
            jnp.maximum, [jnp.max(s, axis=-1, keepdims=True) for s in scores]
        )
        numer = jnp.zeros((B, DH), jnp.float32)
        denom = jnp.zeros((B, 1), jnp.float32)
        for s, v in zip(scores, v_parts):
            w = jnp.exp(s - peak).astype(jnp.bfloat16)
            denom = denom + jnp.sum(w.astype(jnp.float32), axis=-1, keepdims=True)
            numer = numer + jnp.dot(w, v, preferred_element_type=jnp.float32)
        rows = pl.ds(pl.multiple_of(slot_ref[i] * B, B), B)
        out_ref[rows, :] = (numer / denom).astype(out_ref.dtype)

    for i in range(blk_dev):
        pl.when(keep_ref[i] > 0)(functools.partial(one, i))


def attend(keep, slot, live, where, q, k, v, hk, hv, gk, gv, rand):
    tok_dev, width_dev = q.shape
    blk_dev, head_dev = tok_dev // B, width_dev // DH

    def column(rows):
        return pl.BlockSpec((rows, DH), lambda h, *_: (0, h))

    return pl.pallas_call(
        functools.partial(attend_kernel, blk_dev),
        out_shape=jax.ShapeDtypeStruct(q.shape, q.dtype),
        grid_spec=pltpu.PrefetchScalarGridSpec(
            num_scalar_prefetch=4,
            grid=(head_dev,),
            in_specs=[column(tok_dev)] * 3
            + [column(2 * B)] * 2
            + [column(G * B)] * 2
            + [pl.BlockSpec(rand.shape, lambda h, *_: (0, 0, 0, 0))],
            out_specs=column(tok_dev),
        ),
        compiler_params=ANYWHERE,
    )(keep, slot, live, where, q, k, v, hk, hv, gk, gv, rand)


def copy_kernel(order_ref, in_ref, out_ref):
    out_ref[...] = in_ref[...]


def take_blocks(blocks, order, cap):
    width = blocks.shape[1]
    return pl.pallas_call(
        copy_kernel,
        out_shape=jax.ShapeDtypeStruct((cap * B, width), blocks.dtype),
        grid_spec=pltpu.PrefetchScalarGridSpec(
            num_scalar_prefetch=1,
            grid=(cap,),
            in_specs=[pl.BlockSpec((B, width), lambda j, order: (order[j], 0))],
            out_specs=pl.BlockSpec((B, width), lambda j, order: (j, 0)),
        ),
        compiler_params=ANYWHERE,
    )(order, blocks)


def merge_kernel(kind_ref, from_ref, old_ref, new_ref, out_ref):
    kind = kind_ref[pl.program_id(0)]

    @pl.when(kind == 0)
    def _():
        out_ref[...] = old_ref[...]

    @pl.when(kind == 1)
    def _():
        out_ref[...] = jnp.zeros_like(out_ref)

    @pl.when(kind == 2)
    def _():
        out_ref[...] = new_ref[...]


def merge_blocks(old, new, kind, place):
    tok_dev, width = old.shape
    return pl.pallas_call(
        merge_kernel,
        out_shape=jax.ShapeDtypeStruct(old.shape, old.dtype),
        grid_spec=pltpu.PrefetchScalarGridSpec(
            num_scalar_prefetch=2,
            grid=(tok_dev // B,),
            in_specs=[
                pl.BlockSpec((B, width), lambda j, kind, place: (j, 0)),
                pl.BlockSpec((B, width), lambda j, kind, place: (place[j], 0)),
            ],
            out_specs=pl.BlockSpec((B, width), lambda j, kind, place: (j, 0)),
        ),
        compiler_params=ANYWHERE,
    )(kind, place, old, new)


def exclusive(flags, axis):
    return jnp.cumsum(flags, axis=axis) - flags


def first_at_least(caps, amount):
    return jnp.sum((amount > jnp.asarray(caps, jnp.int32)).astype(jnp.int32))


def body(queries, keys, values, random_holder, random_offset, keep):
    tok_dev, width_dev = queries.shape
    blk_dev = tok_dev // B
    head_dev = width_dev // DH
    seq_count = lax.axis_size("seq")
    head_count = lax.axis_size("head")
    me = lax.axis_index("seq")
    count_req = blk_dev * R
    total = head_dev * count_req
    i32 = jnp.int32

    code = random_holder * blk_dev + random_offset
    code = jnp.where((keep > 0)[None, :, None], code, -1).reshape(total)
    note = jnp.concatenate([code, keep])
    note = jnp.broadcast_to(note, (seq_count * head_count,) + note.shape)
    table = lax.all_to_all(note, ("seq", "head"), split_axis=0, concat_axis=0, tiled=True)
    table = table.reshape(seq_count, head_count, total + blk_dev)
    keep_all = table[:, 0, total:].reshape(seq_count * blk_dev)
    codes = table[:, :, :total]
    devices = jnp.arange(seq_count, dtype=i32)

    halo_k, halo_v = halo(keys, "seq", B), halo(values, "seq", B)

    named = jnp.where(codes >= 0, codes // blk_dev, -1)
    counts = jnp.sum((named[..., None] == devices).astype(i32), axis=2)
    most = jnp.max(counts)
    onehot = (named[me, lax.axis_index("head")][:, None] == devices).astype(i32)
    mine = exclusive(onehot, 0)
    my_slot = jnp.sum(mine * onehot, axis=1)
    my_holder = jnp.sum(onehot * devices, axis=1)

    group = codes[:, lax.axis_index("head")]
    asks = (named[:, lax.axis_index("head")] == me).astype(i32)
    order = exclusive(asks, 1)
    full = min(total, head_dev * max(2, (count_req + seq_count - 1) // seq_count))
    chosen = asks[..., None] * (order[..., None] == jnp.arange(full, dtype=i32)).astype(i32)
    ask_head = jnp.arange(total, dtype=i32) // count_req
    ask = jnp.where(group >= 0, group % blk_dev, 0) + ask_head[None] * blk_dev
    ask = jnp.sum(chosen * ask[..., None], axis=1)
    pick_head, pick_block = ask // blk_dev, ask % blk_dev

    rank = exclusive(keep_all, 0)
    slot = rank % blk_dev
    source = jnp.arange(seq_count * blk_dev, dtype=i32) // blk_dev
    distance = jnp.where(keep_all > 0, source - rank // blk_dev, 0)
    my_slots = lax.dynamic_slice_in_dim(slot, me * blk_dev, blk_dev)
    live = jnp.stack([me > 0, me < seq_count - 1]).astype(i32)

    caps = sorted({max(1, full * part // 12) for part in range(8, 13)})

    def gathered(cap):
        def run(q, k, v, hk, hv):
            gk, gv = broadcast(jnp.stack((k[: G * B], v[: G * B])), "seq", 0)
            picked = pick(k, v, pick_head, pick_block, seq_count, cap)
            replies = lax.all_to_all(picked, "seq", split_axis=0, concat_axis=0, tiled=True)
            where = jnp.minimum(my_holder * cap + my_slot, seq_count * cap - 1)
            return attend(keep, my_slots, live, where, q, k, v, hk, hv, gk, gv, replies)

        return run

    blocks = lax.switch(
        first_at_least(caps[:-1], most),
        [gathered(cap) for cap in caps],
        queries, keys, values, halo_k, halo_v,
    )

    slots = jnp.arange(blk_dev, dtype=i32)
    sizes = sorted({0, *range(blk_dev // 2, blk_dev - 1), blk_dev})
    for bit_pos in range((seq_count - 1).bit_length()):
        stride = 2**bit_pos
        at = source - distance % stride
        moving = (keep_all > 0) & (distance // stride % 2 > 0)
        on_slot = ((slot[:, None] == slots) & moving[:, None]).astype(i32)
        on_device = (at[:, None] == devices).astype(i32)
        leaving = jnp.sum(on_device[:, :, None] * on_slot[:, None, :], axis=0)
        needed = jnp.max(jnp.sum(leaving, axis=1))
        nth = exclusive(leaving, 1)
        mine_out, mine_nth = leaving[me], nth[me]
        send = jnp.sum(
            mine_out[:, None] * (mine_nth[:, None] == slots).astype(i32) * slots[:, None], axis=0
        )
        far = jnp.minimum(me + stride, seq_count - 1)
        comes = jnp.where(me + stride < seq_count, leaving[far], 0)
        kind = jnp.where(comes > 0, 2, jnp.where(mine_out > 0, 1, 0)).astype(i32)
        place = jnp.where(comes > 0, nth[far], 0)
        all_pairs = [(i, i - stride) for i in range(stride, seq_count)]
        split = seq_count - stride // 2
        upper = [pair for pair in all_pairs if pair[0] >= split]
        halves = 2 * stride >= seq_count and 0 < len(upper) < len(all_pairs)

        def shifting(cap, pairs, send=send, kind=kind, place=place):
            def run(blocks):
                if cap == 0:
                    return blocks
                moved = lax.ppermute(take_blocks(blocks, send, cap), "seq", pairs)
                return merge_blocks(blocks, moved, kind, jnp.minimum(place, cap - 1))

            return run

        which = first_at_least(sizes[:-1], needed)
        runs = [shifting(cap, all_pairs) for cap in sizes]
        if halves:
            runs += [shifting(cap, upper) for cap in sizes]
            lower = jnp.sum(leaving * (devices < split)[:, None].astype(i32))
            which = which + jnp.where(lower > 0, 0, len(sizes))
        blocks = lax.switch(which, runs, blocks)
    return blocks


def solution(mesh):
    in_specs = (
        P("seq", "head"),
        P("seq", "head"),
        P("seq", "head"),
        P("head", "seq", None),
        P("head", "seq", None),
        P("seq"),
    )
    out_specs = P("seq", "head")
    return jax.shard_map(body, mesh=mesh, in_specs=in_specs, out_specs=out_specs, check_vma=False)
```
